32 devices in a mesh: row: 8 (over z, y), col: 4 (over x, core).
Axes of the slice: x: 2, y: 2, z: 4, core: 2. Of those that a mesh axis runs over, the one named last changes fastest.
Arguments:
- field: float32 [512, 64, 8, 512], P('row', 'col'), may hold values from -6 to 6
- modes: int32 [3, 256], replicated, may hold values from 0 to 511, as said below
Outputs:
- spectrum: float32 [64, 512, 8, 512], P(None, 'col', None, 'row')
- localized: float32 [512, 512], replicated
The draws below stay inside these ranges and needn't reach their ends.
Inputs may be any that keep to these rules, and one draw needn't show every extreme that they name: `modes`: row 0 holds kx in 0 to 255, row 1 ky in 0 to 511, row 2 kz in 0 to 63; triples may repeat.
All inputs are finite; a program needn't handle non-finite values.
Results may differ from the reference program's by a relative error of at most 0.00013.
Values sent between devices are 32-bit elements; how exact they have to be, the bound alone decides.
A program may use at most 192 MiB of HBM per device.

```python
import math
import jax
import jax.numpy as jnp
from jax import lax

NX = 512
NY = 512
NZ = 64
MEMBERS = 8
MODES = 256
REACH = 64


def draw_modes(key, part):
    first_key, second_key, third_key = jax.random.split(jax.random.fold_in(key, 7), 3)
    first = jax.random.randint(first_key, (MODES,), 0, NX // 2)
    second = jax.random.randint(second_key, (MODES,), 0, NY)
    third = jax.random.randint(third_key, (MODES,), 0, NZ)
    return jnp.stack([first, second, third]).astype(jnp.int32)


def steps_of(rng, shape, pieces, least, largest):
    loudness = 1.0
    for dim, parts in pieces:
        heights = jax.random.uniform(jax.random.fold_in(jax.random.fold_in(rng, 6), dim), (parts,), jnp.float32, least / len(pieces), largest / len(pieces))
        loudness = loudness * jnp.repeat(jnp.exp(heights), shape[dim] // parts).reshape((-1,) + (1,) * (len(shape) - 1 - dim))
    return loudness


def bell_draw(rng, extent, scale, reach, cuts=(), kind=jnp.bfloat16):
    entries = jax.random.normal(rng, extent, jnp.float32) * scale
    if len(cuts) > 0:
        entries = steps_of(rng, extent, cuts, -0.22, 0.18) * entries
    return jnp.clip(entries, min=-reach, max=reach).astype(kind)


def setup_inputs(seed: int = 0) -> dict:
    streams_of = jax.random.split(jax.random.key(seed), 3)
    return {
        "field": bell_draw(streams_of[0], (NY, NZ, MEMBERS, NX), 1.0, 6.0, ((0, 8), (1, 4)), jnp.float32),
        "modes": draw_modes(jax.random.fold_in(streams_of[2], 71), 0),
    }


def taper_of(modes):
    first = modes[0].astype(jnp.float32)
    second = jnp.where(modes[1] < NY // 2, modes[1], modes[1] - NY).astype(jnp.float32)
    third = jnp.where(modes[2] < NZ // 2, modes[2], modes[2] - NZ).astype(jnp.float32)
    first = jnp.concatenate([first, first])
    second = jnp.concatenate([second, second])
    third = jnp.concatenate([third, third])
    dist = (first[:, None] - first[None, :]) ** 2 + (second[:, None] - second[None, :]) ** 2
    dist = dist + (third[:, None] - third[None, :]) ** 2
    return jnp.exp(-dist / (2.0 * REACH * REACH))

def covariance_of(coef, modes):
    anomaly = coef - lax.optimization_barrier(jnp.mean(coef, axis=0, keepdims=True))
    cov = jnp.dot(anomaly.T, anomaly, precision=lax.Precision.HIGHEST) / (MEMBERS - 1)
    return cov * taper_of(modes)

def reference(field, modes):
    factor = 1.0 / math.sqrt(NX * NY * NZ)

    def one_member(member):
        whole = jnp.fft.fftn(member)[:, :, :NX // 2] * factor
        whole = jnp.transpose(whole, (1, 0, 2))
        paired = jnp.stack([jnp.real(whole), jnp.imag(whole)], axis=-1)
        return paired.reshape(NZ, NY, NX).astype(jnp.float32)
    stacked = lax.map(one_member, jnp.transpose(field, (2, 0, 1, 3)))
    spectrum = jnp.transpose(stacked, (1, 2, 0, 3))
    real_rows = spectrum[modes[2], modes[1], :, 2 * modes[0]]
    imag_rows = spectrum[modes[2], modes[1], :, 2 * modes[0] + 1]
    coef = jnp.concatenate([real_rows.T, imag_rows.T], axis=1)
    return (spectrum, covariance_of(coef, modes))
```

```python
import math

import jax
import jax.numpy as jnp
from jax import lax
from jax.experimental.layout import Layout, with_layout_constraint
from jax.sharding import PartitionSpec as P

NX = 512
NY = 512
NZ = 64
REACH = 64


highest = lax.Precision.HIGHEST
high = lax.Precision.HIGH
PIECES = 2


def tables(length, count):
    points = lax.iota(jnp.int32, length)
    waves = lax.iota(jnp.int32, count)
    phase = points[:, None] * waves[None, :] % length
    angle = phase.astype(jnp.float32) * (2.0 * math.pi / length)
    return (jnp.cos(angle), jnp.sin(angle))


def taper_of(modes, size_y, size_z, reach):
    first = modes[0].astype(jnp.float32)
    second = jnp.where(modes[1] < size_y // 2, modes[1], modes[1] - size_y).astype(jnp.float32)
    third = jnp.where(modes[2] < size_z // 2, modes[2], modes[2] - size_z).astype(jnp.float32)
    first = jnp.concatenate([first, first])
    second = jnp.concatenate([second, second])
    third = jnp.concatenate([third, third])
    dist = (first[:, None] - first[None, :]) ** 2 + (second[:, None] - second[None, :]) ** 2
    dist = dist + (third[:, None] - third[None, :]) ** 2
    return jnp.exp(-dist / (2.0 * reach * reach))


def twiddle(length, count, scale):
    cos, sin = tables(length, count)
    cos, sin = cos * scale, sin * scale
    return jnp.stack([jnp.stack([cos, sin]), jnp.stack([-sin, cos])])


def per_device(field, modes):
    members = field.shape[2]
    width = field.shape[3]
    rows, cols = lax.axis_size("row"), lax.axis_size("col")
    near, thick = field.shape[0], field.shape[1]
    length, depth = near * rows, thick * cols
    waves = width // 2 // rows
    pieces = PIECES if waves % PIECES == 0 else 1
    part = waves // pieces
    local_y = length // cols
    factor = 1.0 / math.sqrt(NX * NY * NZ)
    cos_x, sin_x = tables(width, width // 2)
    x_table = jnp.stack([cos_x, -sin_x]).reshape(2, width, rows, pieces, part)
    y_table = twiddle(length, length, 1.0).reshape(2, 2, rows, near, length)
    z_table = twiddle(depth, depth, factor).reshape(2, 2, cols, thick, depth)
    flat = field.reshape(near, thick * members, width)
    outs = []
    for piece in range(pieces):
        lines = jnp.einsum("cxrk,ylx->rckyl", x_table[:, :, :, piece], flat, precision=high)
        lines = with_layout_constraint(lines, Layout((0, 1, 2, 3, 4)))
        gathered = lax.all_to_all(lines, "row", split_axis=0, concat_axis=0, tiled=True)
        gathered = with_layout_constraint(gathered, Layout((0, 1, 2, 3, 4)))
        gathered = gathered.reshape(rows, 2, part, near, thick, members)
        ytrans = jnp.einsum("dcsyf,sckyzm->dkmzf", y_table, gathered, precision=high)
        ytrans = ytrans.reshape(2, part, members, thick, cols, local_y)
        ytrans = jnp.transpose(ytrans, (4, 0, 1, 2, 3, 5))
        levels = lax.all_to_all(ytrans, "col", split_axis=0, concat_axis=0, tiled=True)
        outs.append(jnp.einsum("edszg,sdkmzf->gmkef", z_table, levels, precision=high))
    whole = jnp.concatenate(outs, axis=2) if pieces > 1 else outs[0]
    local_q = 2 * waves
    whole = whole.reshape(depth, members, local_q, local_y)
    spectrum = jnp.transpose(whole, (0, 3, 1, 2))
    row_start = lax.axis_index("row") * waves
    col_start = lax.axis_index("col") * local_y
    wave = modes[0] - row_start
    line = modes[1] - col_start
    inside = (wave >= 0) & (wave < waves) & (line >= 0) & (line < local_y)
    wave = jnp.clip(wave, 0, waves - 1)
    line = jnp.clip(line, 0, local_y - 1)
    columns = lax.iota(jnp.int32, local_y)
    tall = whole.reshape(depth, members, waves, 2, local_y)
    picked = tall[modes[2], :, wave]
    hit = (columns[None, :] == line[:, None]) & inside[:, None]
    value = jnp.sum(jnp.where(hit[:, None, None, :], picked, 0.0), axis=-1)
    partial_value = jnp.transpose(value, (1, 2, 0)).reshape(members, -1)
    coef = lax.psum(partial_value, ("row", "col"))
    anomaly = coef - jnp.mean(coef, axis=0, keepdims=True)
    cov = jnp.dot(anomaly.T, anomaly, precision=highest) / (members - 1)
    localized = cov * taper_of(modes, NY, NZ, REACH)
    return (spectrum, localized)


def solution(mesh):
    placed = (P("row", "col", None, None), P())
    return jax.shard_map(
        per_device,
        mesh=mesh,
        in_specs=placed,
        out_specs=(P(None, "col", None, "row"), P()),
        check_vma=False,
    )
```
